32 devices in a mesh: dp: 2 (over x), ep: 16 (over z, y, core).
Axes of the slice: x: 2, y: 2, z: 4, core: 2. Of those that a mesh axis runs over, the one named last changes fastest.
Arguments:
- tokens: bfloat16 [262144, 768], P(('dp', 'ep')), parts along dimension 0
- expert_idx: int32 [262144], P(('dp', 'ep')), parts along dimension 0
- w_router: float32 [768, 32], replicated
- w_in: bfloat16 [32, 768, 3072], P('ep')
- w_out: bfloat16 [32, 3072, 768], P('ep')
Outputs:
- output: bfloat16 [262144, 768], P(('dp', 'ep')), parts along dimension 0
There are 2 independent parts. The reference program is written for one: setup_inputs(seed, part) draws one part's arguments, and reference() takes and returns one part's arrays. A program takes and returns all parts, laid end to end along the dimension named above; an argument that names none is the same for every part.
All inputs are finite; a program needn't handle non-finite values.
Results may differ from the reference program's by a relative error of at most 0.001.
Values are sent between devices in bfloat16 or wider.
A program may use at most 1 GiB of HBM per device.

```python
import jax
import jax.numpy as jnp
from jax import lax

MODEL_DIM = 768
HIDDEN_DIM = 3072
NUM_EXPERTS = 32
GROUP_TOKENS = 8192
NUM_GROUPS = 16
CAPACITY = (5 * GROUP_TOKENS + 4 * NUM_EXPERTS - 1) // (4 * NUM_EXPERTS)
TOTAL_TOKENS = NUM_GROUPS * GROUP_TOKENS


def draw_choices(key):
    key_perm, key_shift, key_redraw, key_pick, key_hot = jax.random.split(key, 5)
    balanced = jnp.arange(GROUP_TOKENS, dtype=jnp.int32) % NUM_EXPERTS
    perm_keys = jax.random.split(key_perm, NUM_GROUPS)
    shuffled = jax.vmap(lambda perm_key: jax.random.permutation(perm_key, balanced))(perm_keys)
    group_shift = jax.random.randint(key_shift, (NUM_GROUPS, 1), 0, NUM_EXPERTS)
    choice = (shuffled + group_shift) % NUM_EXPERTS
    redraw = jax.random.randint(key_redraw, (NUM_GROUPS, GROUP_TOKENS), 0, 8) == 0
    picked = jax.random.randint(key_pick, (NUM_GROUPS, GROUP_TOKENS), 0, NUM_EXPERTS)
    choice = jnp.where(redraw, picked, choice)
    hot_expert = jax.random.randint(key_hot, (NUM_GROUPS, 1), 0, NUM_EXPERTS)
    leading = jnp.arange(GROUP_TOKENS)[None, :] <= CAPACITY
    choice = jnp.where(leading, hot_expert, choice)
    return choice.reshape(TOTAL_TOKENS).astype(jnp.int32)


def expert_weights(key, fan_in, fan_out, weight_scale):
    expert_keys = jax.random.split(key, NUM_EXPERTS)
    return lax.map(lambda one_key: (jax.random.normal(one_key, (fan_in, fan_out), jnp.float32) * weight_scale).astype(jnp.bfloat16), expert_keys)


def setup_inputs(seed: int = 0, part: int = 0) -> dict:
    root_key = jax.random.key(seed)
    key_tokens, key_choice, key_router, key_in, key_out = jax.random.split(root_key, 5)
    tokens = jax.random.normal(jax.random.fold_in(key_tokens, part), (TOTAL_TOKENS, MODEL_DIM), jnp.float32).astype(jnp.bfloat16)
    expert_idx = draw_choices(jax.random.fold_in(key_choice, part))
    w_router = jax.random.normal(key_router, (MODEL_DIM, NUM_EXPERTS), jnp.float32) * MODEL_DIM ** -0.5
    w_in = expert_weights(key_in, MODEL_DIM, HIDDEN_DIM, MODEL_DIM ** -0.5)
    w_out = expert_weights(key_out, HIDDEN_DIM, MODEL_DIM, NUM_EXPERTS * HIDDEN_DIM ** -0.5)
    return {"tokens": tokens, "expert_idx": expert_idx, "w_router": w_router, "w_in": w_in, "w_out": w_out}


def route_group(tok_rows, choice, w_router):
    logits = jnp.dot(tok_rows.astype(jnp.float32), w_router, precision=lax.Precision.HIGHEST)
    router_prob = jax.nn.softmax(logits, axis=-1)
    chosen = choice[:, None] == jnp.arange(NUM_EXPERTS, dtype=jnp.int32)[None, :]
    gate_prob = jnp.sum(jnp.where(chosen, router_prob, 0.0), axis=-1)
    running_count = jnp.cumsum(chosen.astype(jnp.int32), axis=0) - 1
    position = jnp.sum(jnp.where(chosen, running_count, 0), axis=-1)
    slot_index = jnp.where(position < CAPACITY, choice * CAPACITY + position, NUM_EXPERTS * CAPACITY)
    holder = jnp.full((NUM_EXPERTS * CAPACITY + 1,), GROUP_TOKENS, jnp.int32).at[slot_index].set(jnp.arange(GROUP_TOKENS, dtype=jnp.int32))
    buffer = jnp.take(tok_rows, holder[:-1], axis=0, mode="fill", fill_value=0)
    return buffer.reshape(NUM_EXPERTS, CAPACITY, MODEL_DIM), slot_index, gate_prob


def expert_apply(operands):
    rows_in, weight_in, weight_out = operands
    hidden = jnp.dot(rows_in, weight_in, preferred_element_type=jnp.float32)
    hidden_act = jax.nn.relu(hidden).astype(jnp.bfloat16)
    return jnp.dot(hidden_act, weight_out, preferred_element_type=jnp.float32).astype(jnp.bfloat16)


def combine_group(operands):
    flat_out, slot_rows, gate_rows = operands
    picked = jnp.take(flat_out, slot_rows, axis=0, mode="fill", fill_value=0)
    return (gate_rows[:, None] * picked.astype(jnp.float32)).astype(jnp.bfloat16)


def reference(tokens, expert_idx, w_router, w_in, w_out):
    grouped = tokens.reshape(NUM_GROUPS, GROUP_TOKENS, MODEL_DIM)
    choices = expert_idx.reshape(NUM_GROUPS, GROUP_TOKENS)
    buffers, slot_index, gate_prob = lax.map(lambda pair: route_group(pair[0], pair[1], w_router), (grouped, choices))
    per_expert = jnp.swapaxes(buffers, 0, 1).reshape(NUM_EXPERTS, NUM_GROUPS * CAPACITY, MODEL_DIM)
    expert_rows = lax.map(expert_apply, (per_expert, w_in, w_out))
    by_group = jnp.swapaxes(expert_rows.reshape(NUM_EXPERTS, NUM_GROUPS, CAPACITY, MODEL_DIM), 0, 1).reshape(NUM_GROUPS, NUM_EXPERTS * CAPACITY, MODEL_DIM)
    outputs = lax.map(combine_group, (by_group, slot_index, gate_prob))
    return outputs.reshape(TOTAL_TOKENS, MODEL_DIM)
```

```python
import jax
import jax.numpy as jnp
from jax import lax
from jax.experimental import pallas as pl
from jax.experimental.pallas import tpu as pltpu
from jax.sharding import PartitionSpec as P


AXES = ("dp", "ep")


def lin(x, z, y, c):
    return x * 16 + z * 4 + y * 2 + c


DEVICES = [(x, z, y, c) for x in range(2) for z in range(4) for y in range(2) for c in range(2)]


def ffn_body(kind, n, *refs):
    x_refs = refs[:n]
    w_in_ref, w_out_ref = refs[n], refs[n + 1]
    o_refs = refs[n + 2:2 * n + 2]
    rows_ref, acc_ref = refs[2 * n + 2:]
    step = pl.program_id(0)
    cap = o_refs[0].shape[0]

    @pl.when(step == 0)
    def _():
        for i in range(n):
            rows_ref[pl.ds(i * cap, cap), :] = x_refs[i][0]

    half = n * cap // 2
    for part in range(2):
        span = pl.ds(part * half, half)
        hidden = jnp.dot(rows_ref[span, :], w_in_ref[...], preferred_element_type=jnp.float32)
        hidden = jnp.maximum(hidden, 0.0).astype(jnp.bfloat16)
        term = jnp.dot(hidden, w_out_ref[...], preferred_element_type=jnp.float32)

        @pl.when(step == 0)
        def _():
            acc_ref[span, :] = term

        @pl.when(step > 0)
        def _():
            acc_ref[span, :] += term

    @pl.when(step == pl.num_programs(0) - 1)
    def _():
        for i in range(n):
            o_refs[i][...] = acc_ref[pl.ds(i * cap, cap), :].astype(jnp.bfloat16)


def ffn(chunks, kind, w_in, w_out, tile=512):
    n = len(chunks)
    cap, dim = chunks[0].shape[1:]
    hid = w_in.shape[1]
    row_spec = pl.BlockSpec((1, cap, dim), lambda f: (kind, 0, 0))
    return pl.pallas_call(
        lambda *refs: ffn_body(kind, n, *refs),
        grid=(hid // tile,),
        in_specs=[row_spec] * n + [pl.BlockSpec((dim, tile), lambda f: (0, f)), pl.BlockSpec((tile, dim), lambda f: (f, 0))],
        out_specs=[pl.BlockSpec((cap, dim), lambda f: (0, 0))] * n,
        out_shape=[jax.ShapeDtypeStruct((cap, dim), jnp.bfloat16)] * n,
        scratch_shapes=[pltpu.VMEM((n * cap, dim), jnp.bfloat16), pltpu.VMEM((n * cap, dim), jnp.float32)],
        compiler_params=pltpu.CompilerParams(dimension_semantics=("arbitrary",), vmem_limit_bytes=60 << 20),
        cost_estimate=pl.CostEstimate(flops=4 * n * cap * dim * hid, bytes_accessed=4 * (dim * hid + n * cap * dim), transcendentals=0),
        name=f"ffn{kind}",
    )(*chunks, w_in, w_out)


def solution(mesh):
    def permute(value, pairs):
        return lax.ppermute(value, AXES, [(lin(*a), lin(*b)) for a, b in pairs])

    def flip(mask, dev, z):
        x, _, y, c = dev
        return (x ^ (mask >> 2), z, y ^ ((mask >> 1) & 1), c ^ (mask & 1))

    def in_half(z):
        return 1 if z < 2 else 2

    def local_block(tokens, expert_idx, w_router, w_in, w_out):
        tok_count, dim = tokens.shape
        num_experts = w_router.shape[1]
        capacity = (5 * tok_count + 4 * num_experts - 1) // (4 * num_experts)
        x = lax.axis_index("dp")
        ep = lax.axis_index("ep")
        z, y, c = ep // 4, (ep // 2) % 2, ep % 2

        swap_near = [(d, (d[0], d[1] ^ 1, d[2], d[3])) for d in DEVICES]
        swap_mid = [(d, (d[0], 3 - d[1], d[2], d[3])) for d in DEVICES if d[1] in (1, 2)]
        wa = (lax.dynamic_index_in_dim(w_in, x, 0, False), lax.dynamic_index_in_dim(w_out, x, 0, False))
        wb = tuple(permute(w, swap_near) for w in wa)
        wc = tuple(permute(w, swap_mid) for w in wa)
        wd = tuple(permute(w, swap_mid) for w in wb)

        logits = jnp.dot(tokens.astype(jnp.float32), w_router, precision=lax.Precision.HIGHEST)
        router_prob = jax.nn.softmax(logits, axis=-1)
        chosen = expert_idx[:, None] == jnp.arange(num_experts, dtype=jnp.int32)[None, :]
        gate = jnp.sum(jnp.where(chosen, router_prob, 0.0), axis=-1)
        running = jnp.cumsum(chosen.astype(jnp.int32), axis=0) - 1
        position = jnp.sum(jnp.where(chosen, running, 0), axis=-1)

        bit_x, bit_c, bit_y, slab = expert_idx & 1, (expert_idx >> 1) & 1, (expert_idx >> 2) & 1, expert_idx >> 3
        mask = ((bit_x ^ x) << 2) | ((bit_y ^ y) << 1) | (bit_c ^ c)
        far = (slab >> 1) != (z >> 1)
        second = jnp.where(far, (slab == 0) | (slab == 3), slab != z)
        block = far.astype(jnp.int32) * 16 + mask * 2 + second.astype(jnp.int32)
        kept = position < capacity
        slot = jnp.where(kept, block * capacity + position, num_experts * capacity)
        holder = jnp.zeros((num_experts * capacity + 1,), jnp.int32).at[slot].set(jnp.arange(tok_count, dtype=jnp.int32))

        def chunk(k):
            rows = lax.slice(holder, (k * 2 * capacity,), ((k + 1) * 2 * capacity,))
            return jnp.take(tokens, rows, axis=0, mode="clip").reshape(2, capacity, dim)

        order = [7, 6, 5, 3, 4, 2, 1, 0]
        near_pairs = {m: [(d, flip(m, d, d[1])) for d in DEVICES] for m in range(8)}
        inner_pairs = {m: [p for p in near_pairs[m] if p[0][1] in (1, 2)] for m in range(8)}
        outer_pairs = {m: [(d, flip(m, d, in_half(d[1]))) for d in DEVICES if d[1] in (0, 3)] for m in range(8)}
        back_pairs = {m: [(b, a) for a, b in outer_pairs[m]] for m in range(8)}

        near_out = {m: chunk(m) for m in order}
        near_in = {m: permute(near_out[m], near_pairs[m]) if m else near_out[m] for m in order}
        far_out = {m: chunk(8 + m) for m in order}
        edge_in = {m: permute(far_out[m], outer_pairs[m]) for m in order}
        far_in = {m: permute(far_out[m], inner_pairs[m]) if m else far_out[m] for m in order}

        back = {}

        def run(tag, source, kind, weights, pairs):
            outs = ffn([source[m] for m in order], kind, *weights)
            for m, out in zip(order, outs):
                back[tag, m] = out if pairs[m] is None else permute(out, pairs[m])

        near_back = {m: near_pairs[m] if m else None for m in order}
        inner_back = {m: inner_pairs[m] if m else None for m in order}
        run("a", near_in, 0, wa, near_back)
        run("b", near_in, 1, wb, near_back)
        run("ce", edge_in, 0, wc, back_pairs)
        run("ci", far_in, 0, wc, inner_back)
        run("de", edge_in, 1, wd, back_pairs)
        run("di", far_in, 1, wd, inner_back)

        parts = [back[t, m] for m in range(8) for t in ("a", "b")]
        parts += [back[t, m] for m in range(8) for t in ("ci", "di")]
        parts += [back[t, m] for m in range(8) for t in ("ce", "de")]
        flat = jnp.concatenate(parts, axis=0)
        is_edge = (z == 0) | (z == 3)
        source_row = jnp.where(kept, slot + jnp.where(far & is_edge, 16 * capacity, 0), 0)
        picked = jnp.take(flat, source_row, axis=0, mode="clip")
        scaled = (gate[:, None] * picked.astype(jnp.float32)).astype(jnp.bfloat16)
        return jnp.where(kept[:, None], scaled, jnp.zeros_like(scaled))

    return jax.shard_map(local_block, mesh=mesh, in_specs=(P(AXES, None), P(AXES), P(None, None), P("ep", None, None), P("ep", None, None)), out_specs=P(AXES, None), check_vma=False)
```

```python
import jax
import jax.numpy as jnp
from jax import lax
from jax.experimental import pallas as pl
from jax.experimental.pallas import tpu as pltpu
from jax.sharding import PartitionSpec as P

AXES = ("dp", "ep")
MESH = pl.DeviceIdType.MESH
PAIRS = 4


def exchange_body(disp, w_in, w_out, wb_in, wc_in,
                  back, wb_out, wc_out, wd_in, wd_out,
                  xs, wi, wo, hid, x_send, x_recv, w_send, w_recv, r_send, b_recv, w_load):
    x = lax.axis_index("dp")
    ep = lax.axis_index("ep")
    z, y, c = ep // 4, (ep // 2) % 2, ep % 2
    inner = (z == 1) | (z == 2)
    z_near = z + 1 - 2 * (z % 2)
    z_mid = 3 - z

    def device(m, slab):
        return ((x + m // 4) % 2, slab * 4 + ((y + (m // 2) % 2) % 2) * 2 + (c + m % 2) % 2)

    def remote(src, dst, send, recv, dev):
        return pltpu.make_async_remote_copy(src, dst, send, recv, device_id=dev, device_id_type=MESH)

    barrier = pltpu.get_barrier_semaphore()
    for m in range(1, 8):
        pl.semaphore_signal(barrier, inc=1, device_id=device(m, z), device_id_type=MESH)
    for m in range(8):
        pl.semaphore_signal(barrier, inc=1, device_id=device(m, z_near), device_id_type=MESH)
    pl.semaphore_signal(barrier, inc=1, device_id=device(0, z_mid), device_id_type=MESH)
    pl.semaphore_wait(barrier, 16)

    send_b = remote(w_out.at[x], wb_out, w_send.at[0], w_recv.at[0], device(0, z_near))
    send_c = remote(w_out.at[x], wc_out, w_send.at[1], w_recv.at[1], device(0, z_mid))
    send_di = remote(wb_in, wd_in, w_send.at[2], w_recv.at[2], device(0, z_mid))
    send_do = remote(wb_out, wd_out, w_send.at[3], w_recv.at[3], device(0, z_mid))

    def load(src, dst, k):
        return pltpu.make_async_copy(src, dst, w_load.at[k])

    load_a = (load(w_in.at[x], wi.at[0], 0), load(w_out.at[x], wo.at[0], 1))
    load_b = (load(wb_in, wi.at[1], 2), load(wb_out, wo.at[1], 3))
    load_c = (load(wc_in, wi.at[0], 0), load(wc_out, wo.at[0], 1))
    load_d = (load(wd_in, wi.at[1], 2), load(wd_out, wo.at[1], 3))

    send_b.start()

    @pl.when(inner)
    def _():
        send_c.start()
        send_di.start()

    def own(q, r):
        return pltpu.make_async_copy(disp.at[q, 0], xs.at[r, 0], x_recv.at[r, 0])

    def dispatch(q, r, m, slab):
        return remote(disp.at[q, m], xs.at[r, m], x_send.at[q, m], x_recv.at[r, m], device(m, slab))

    for copy in load_a:
        copy.start()
    load_b[0].start()
    own(0, 0).start()
    own(1, 1).start()

    order = (1, 2, 4, 3, 5, 6, 7)
    for m in order:
        dispatch(0, 0, m, z).start()
    for m in order:
        dispatch(1, 1, m, z).start()

    @pl.when(inner)
    def _():
        own(2, 2).start()
        own(3, 5).start()
        for m in order:
            dispatch(2, 2, m, z).start()
        for m in order:
            dispatch(3, 5, m, z).start()

    @pl.when(jnp.logical_not(inner))
    def _():
        for m in range(8):
            dispatch(2, 3, m, z_near).start()
        for m in range(8):
            dispatch(3, 4, m, z_near).start()

    cap, dim = xs.shape[2:]
    hidden = wi.shape[2]
    rows = 2 * cap
    tile_in, tile_out = 512, 256

    def compute(r, p, b):
        view = xs.at[r]

        def first(n, carry):
            cols = pl.ds(pl.multiple_of(n * tile_in, tile_in), tile_in)
            value = jnp.dot(view[pl.ds(2 * p, 2)].reshape(rows, dim), wi[b, :, cols], preferred_element_type=jnp.float32)
            hid[:, cols] = jnp.maximum(value, 0.0).astype(jnp.bfloat16)
            return carry

        lax.fori_loop(0, hidden // tile_in, first, 0)

        def second(n, carry):
            cols = pl.ds(pl.multiple_of(n * tile_out, tile_out), tile_out)
            value = jnp.dot(hid[...], wo[b, :, cols], preferred_element_type=jnp.float32)
            view[pl.ds(2 * p, 2), :, cols] = value.astype(jnp.bfloat16).reshape(2, cap, tile_out)
            return carry

        lax.fori_loop(0, dim // tile_out, second, 0)

    def landed(sem):
        pltpu.make_async_copy(xs.at[0, 0], xs.at[0, 0], sem).wait()

    def job(j, carry):
        r, p = j // PAIRS, j % PAIRS

        @pl.when(j == 0)
        def _():
            load_a[0].wait()
            load_a[1].wait()

        @pl.when(j == PAIRS)
        def _():
            send_b.wait_recv()
            load_b[1].start()

            @pl.when(inner)
            def _():
                send_do.start()
                load_c[0].start()

            load_b[0].wait()
            load_b[1].wait()

        @pl.when(j == 2 * PAIRS)
        def _():
            send_c.wait_recv()
            load_c[1].start()
            load_c[0].wait()
            load_c[1].wait()

        @pl.when(j == 4 * PAIRS)
        def _():
            send_di.wait_recv()
            load_d[0].start()
            send_do.wait_recv()
            load_d[1].start()
            load_d[0].wait()
            load_d[1].wait()

        landed(x_recv.at[r, 2 * p])
        landed(x_recv.at[r, 2 * p + 1])
        late = r // 4
        kind = jnp.where(r == 1, 1, late)
        compute(r, p, kind)
        edge = (r == 3) | (r == 4)
        q = jnp.where(r < 2, 0, 2) + kind
        slab = jnp.where(edge, z_near, z)

        def result(m):
            return remote(xs.at[r, m], back.at[q, m], r_send.at[r, m], b_recv.at[q, m], device(m, slab))

        keep = (p == 0) & jnp.logical_not(edge)

        @pl.when(keep)
        def _():
            pltpu.make_async_copy(xs.at[r, 0], back.at[q, 0], b_recv.at[q, 0]).start()

        @pl.when(jnp.logical_not(keep))
        def _():
            result(2 * p).start()

        result(2 * p + 1).start()
        return carry

    lax.fori_loop(0, jnp.where(inner, 6 * PAIRS, 2 * PAIRS), job, 0)

    def each(fn, lo, hi):
        def step(i, carry):
            fn(i)
            return carry

        lax.fori_loop(lo, hi, step, 0)

    skip = jnp.where(inner, 1, 0)
    for q in range(4):
        each(lambda m: landed(b_recv.at[q, m]), 0, 8)
        each(lambda m: landed(x_send.at[q, m]), 1 if q < 2 else skip, 8)
    for r in (0, 1):
        each(lambda m: landed(r_send.at[r, m]), 1, 8)
    send_b.wait_send()

    @pl.when(inner)
    def _():
        for r in (2, 3, 4, 5):
            each(lambda m: landed(r_send.at[r, m]), 0 if r in (3, 4) else 1, 8)
        send_c.wait_send()
        send_di.wait_send()
        send_do.wait_send()


def exchange(disp, w_in, w_out, wb_in, wc_in):
    _, _, cap, dim = disp.shape
    hidden = w_in.shape[2]
    anywhere = pl.BlockSpec(memory_space=pl.ANY)
    dma = pltpu.SemaphoreType.DMA
    bf16 = jnp.bfloat16
    in_shape, out_shape = (dim, hidden), (hidden, dim)
    outs = [disp.shape, out_shape, out_shape, in_shape, out_shape]
    return pl.pallas_call(
        exchange_body,
        in_specs=[anywhere] * 5,
        out_specs=[anywhere] * 5,
        out_shape=[jax.ShapeDtypeStruct(s, bf16) for s in outs],
        scratch_shapes=[
            pltpu.VMEM((6, 8, cap, dim), bf16),
            pltpu.VMEM((2,) + in_shape, bf16),
            pltpu.VMEM((2,) + out_shape, bf16),
            pltpu.VMEM((2 * cap, hidden), bf16),
            dma((4, 8)), dma((6, 8)), dma((4,)), dma((4,)), dma((6, 8)), dma((4, 8)), dma((4,)),
        ],
        compiler_params=pltpu.CompilerParams(collective_id=0, has_side_effects=True, vmem_limit_bytes=60 << 20),
        cost_estimate=pl.CostEstimate(flops=4 * 48 * cap * dim * hidden, bytes_accessed=100 << 20, transcendentals=0),
        name="exchange",
    )(disp, w_in, w_out, wb_in, wc_in)[0]


def lin(x, z, y, c):
    return x * 16 + z * 4 + y * 2 + c


DEVICES = [(x, z, y, c) for x in range(2) for z in range(4) for y in range(2) for c in range(2)]


def solution(mesh):
    swap_near = [(lin(x, z, y, c), lin(x, z ^ 1, y, c)) for x, z, y, c in DEVICES]
    swap_mid = [(lin(x, z, y, c), lin(x, 3 - z, y, c)) for x, z, y, c in DEVICES if z in (1, 2)]

    def local_block(tokens, expert_idx, w_router, w_in, w_out):
        tok_count, dim = tokens.shape
        num_experts = w_router.shape[1]
        capacity = (5 * tok_count + 4 * num_experts - 1) // (4 * num_experts)
        x = lax.axis_index("dp")
        ep = lax.axis_index("ep")
        z, y, c = ep // 4, (ep // 2) % 2, ep % 2

        wa_in = lax.dynamic_index_in_dim(w_in, x, 0, False)
        with jax.named_scope("weights_mid"):
            wc_in = lax.ppermute(wa_in, AXES, swap_mid)
        with jax.named_scope("weights_near"):
            wb_in = lax.ppermute(wa_in, AXES, swap_near)

        logits = jnp.dot(tokens.astype(jnp.float32), w_router, precision=lax.Precision.HIGHEST)
        router_prob = jax.nn.softmax(logits, axis=-1)
        chosen = expert_idx[:, None] == jnp.arange(num_experts, dtype=jnp.int32)[None, :]
        gate = jnp.sum(jnp.where(chosen, router_prob, 0.0), axis=-1)
        running = jnp.cumsum(chosen.astype(jnp.int32), axis=0) - 1
        position = jnp.sum(jnp.where(chosen, running, 0), axis=-1)

        bit_x, bit_c, bit_y, slab = expert_idx & 1, (expert_idx >> 1) & 1, (expert_idx >> 2) & 1, expert_idx >> 3
        mask = ((bit_x ^ x) << 2) | ((bit_y ^ y) << 1) | (bit_c ^ c)
        far = (slab >> 1) != (z >> 1)
        second = jnp.where(far, (slab == 0) | (slab == 3), slab != z)
        block = far.astype(jnp.int32) * 16 + second.astype(jnp.int32) * 8 + mask
        kept = position < capacity
        slot = jnp.where(kept, block * capacity + position, num_experts * capacity)
        holder = jnp.zeros((num_experts * capacity + 1,), jnp.int32).at[slot].set(jnp.arange(tok_count, dtype=jnp.int32))
        disp = jnp.take(tokens, holder[:-1], axis=0, mode="clip").reshape(4, 8, capacity, dim)

        back = exchange(disp, w_in, w_out, wb_in, wc_in)

        picked = jnp.take(back.reshape(num_experts * capacity, dim), jnp.where(kept, slot, 0), axis=0, mode="clip")
        scaled = (gate[:, None] * picked.astype(jnp.float32)).astype(jnp.bfloat16)
        return jnp.where(kept[:, None], scaled, jnp.zeros_like(scaled))

    return jax.shard_map(local_block, mesh=mesh, in_specs=(P(AXES, None), P(AXES), P(None, None), P("ep", None, None), P("ep", None, None)), out_specs=P(AXES, None), check_vma=False)
```

```python
import jax
import jax.numpy as jnp
from jax import lax
from jax.experimental import pallas as pl
from jax.experimental.pallas import tpu as pltpu
from jax.sharding import PartitionSpec as P

AXES = ("dp", "ep")
MESH = pl.DeviceIdType.MESH
PAIRS = 4


def exchange_body(disp, w_in, w_out, wb_in, wc_in,
                  back, wb_out, wc_out, wd_in, wd_out, relay,
                  xs, wi, wo, hid, x_send, x_recv, w_send, w_recv, r_send, b_recv, w_load, relay_recv, relay_send):
    x = lax.axis_index("dp")
    ep = lax.axis_index("ep")
    z, y, c = ep // 4, (ep // 2) % 2, ep % 2
    inner = (z == 1) | (z == 2)
    outer = jnp.logical_not(inner)
    z_near = z + 1 - 2 * (z % 2)
    z_mid = 3 - z
    cap, dim = xs.shape[2:]
    hidden = wi.shape[2]
    tiles, tile_out = wo.shape[1], wo.shape[3]
    rows = 2 * cap
    tile_in = 512

    def device(m, slab):
        return ((x + m // 4) % 2, slab * 4 + ((y + (m // 2) % 2) % 2) * 2 + (c + m % 2) % 2)

    def remote(src, dst, send, recv, dev):
        return pltpu.make_async_remote_copy(src, dst, send, recv, device_id=dev, device_id_type=MESH)

    barrier = pltpu.get_barrier_semaphore()
    for m in range(1, 8):
        pl.semaphore_signal(barrier, inc=1, device_id=device(m, z), device_id_type=MESH)
    for m in range(8):
        pl.semaphore_signal(barrier, inc=1, device_id=device(m, z_near), device_id_type=MESH)
    pl.semaphore_signal(barrier, inc=1, device_id=device(0, z_mid), device_id_type=MESH)
    pl.semaphore_wait(barrier, 16)

    def cols(t):
        return pl.ds(t * tile_out, tile_out)

    def weight(src, dst, k, slab):
        return remote(src, dst, w_send.at[k], w_recv.at[k], device(0, slab))

    send_b = [weight(w_out.at[x, :, cols(t)], wb_out.at[t], t, z_near) for t in range(tiles)]
    send_c = [weight(w_out.at[x, :, cols(t)], wc_out.at[t], 3 + t, z_mid) for t in range(tiles)]
    send_di = weight(wb_in, wd_in, 6, z_mid)
    send_do = [weight(wb_out.at[t], wd_out.at[t], 7 + t, z_mid) for t in range(tiles)]

    def load(src, dst, k):
        return pltpu.make_async_copy(src, dst, w_load.at[k])

    load_a = [load(w_in.at[x], wi.at[0], 0)] + [load(w_out.at[x, :, cols(t)], wo.at[0, t], 1 + t) for t in range(tiles)]
    load_b = [load(wb_in, wi.at[0], 0), load(wb_out, wo.at[0], 1)]
    load_c = [load(wc_in, wi.at[1], 4), load(wc_out, wo.at[1], 5)]
    load_di = load(wd_in, wi.at[1], 4)
    load_do = [load(wd_out.at[t], wo.at[1, t], 5 + t) for t in range(tiles)]

    def landed(sem):
        pltpu.make_async_copy(xs.at[0, 0], xs.at[0, 0], sem).wait()

    def own(q, r):
        return pltpu.make_async_copy(disp.at[q, 0], xs.at[r, 0], x_recv.at[r, 0])

    def dispatch(q, r, m, slab):
        return remote(disp.at[q, m], xs.at[r, m], x_send.at[q, m], x_recv.at[r, m], device(m, slab))

    @pl.when(inner)
    def _():
        for copy in send_b + send_c + [send_di]:
            copy.start()

    def hand(k, m):
        return remote(disp.at[2 + k, m], relay.at[k, m], x_send.at[2 + k, m], relay_recv.at[k, m], device(m, z))

    def forward(k, m):
        src = relay.at[k, m] if m else disp.at[2 + k, 0]
        return remote(src, xs.at[2 + 2 * k, m], relay_send.at[k, m], x_recv.at[2 + 2 * k, m], device(0, z_near))

    order = (1, 2, 4, 3, 5, 6, 7)

    @pl.when(outer)
    def _():
        for m in order:
            hand(0, m).start()
        forward(0, 0).start()
        send_b[0].start()

    own(0, 0).start()
    own(1, 3).start()
    for copy in load_a:
        copy.start()

    for m in order:
        dispatch(0, 0, m, z).start()

    @pl.when(inner)
    def _():
        load_c[0].start()
        own(2, 1).start()
        own(3, 5).start()
        for m in order:
            dispatch(2, 1, m, z).start()

    @pl.when(outer)
    def _():
        for m in order:
            hand(1, m).start()

    for m in order:
        dispatch(1, 3, m, z).start()

    @pl.when(inner)
    def _():
        for m in order:
            dispatch(3, 5, m, z).start()

    def pass_on(k, m):
        landed(relay_recv.at[k, m])
        forward(k, m).start()

    @pl.when(outer)
    def _():
        for m in order:
            pass_on(0, m)
        send_b[1].start()
        send_b[2].start()

    def first(r, p, b, kept):
        view = xs.at[r]

        def step(n, carry):
            span = pl.ds(pl.multiple_of(n * tile_in, tile_in), tile_in)
            value = jnp.dot(view[pl.ds(2 * p, 2)].reshape(rows, dim), wi[b, :, span], preferred_element_type=jnp.float32)
            kept[:, span] = jnp.maximum(value, 0.0).astype(jnp.bfloat16)
            return carry

        lax.fori_loop(0, hidden // tile_in, step, 0)

    def second(r, p, b, kept, t):
        value = jnp.dot(kept[...], wo[b, t], preferred_element_type=jnp.float32)
        span = pl.ds(pl.multiple_of(t * tile_out, tile_out), tile_out)
        xs[r, pl.ds(2 * p, 2), :, span] = value.astype(jnp.bfloat16).reshape(2, cap, tile_out)

    def each(lo, hi, fn):
        def step(i, carry):
            fn(i)
            return carry

        lax.fori_loop(lo, hi, step, 0)

    def send_back(r, q, p, edge):
        slab = jnp.where(edge, z_near, z)

        def result(m):
            return remote(xs.at[r, m], back.at[q, m], r_send.at[r, m], b_recv.at[q, m], device(m, slab))

        keep = (p == 0) & jnp.logical_not(edge)

        @pl.when(keep)
        def _():
            pltpu.make_async_copy(xs.at[r, 0], back.at[q, 0], b_recv.at[q, 0]).start()

        @pl.when(jnp.logical_not(keep))
        def _():
            result(2 * p).start()

        result(2 * p + 1).start()

    def whole(r, q, p, b, edge):
        landed(x_recv.at[r, 2 * p])
        landed(x_recv.at[r, 2 * p + 1])
        first(r, p, b, hid.at[0])
        each(0, tiles, lambda t: second(r, p, b, hid.at[0], t))
        send_back(r, q, p, edge)

    def late_step(s):
        is_first = (s < 4) | (s == 8) | (s == 13)
        k = jnp.where(s < 2, 4 + s, jnp.where(s < 6, s % 2, jnp.where(s < 8, s - 2, jnp.where(s < 10, 2, jnp.where(s < 13, s - 10, jnp.where(s < 16, 3, jnp.where(s < 18, s - 12, s % 6)))))))
        t = jnp.where((s < 10) | (s == 14), 0, jnp.where(s < 18, 1, 2))
        edge = k < 4
        r = jnp.where(edge, 4, 5)
        p = jnp.where(edge, k, 7 - k)
        slab = jnp.where(edge, z_near, z)
        spare = wi.at[0, pl.ds(0, rows)]

        for step, tile in ((4, 0), (10, 1), (18, 2)):
            @pl.when(s == step)
            def _():
                send_do[tile].wait_recv()
                load_do[tile].start()
                load_do[tile].wait()

        @pl.when(is_first)
        def _():
            landed(x_recv.at[r, 2 * p])
            landed(x_recv.at[r, 2 * p + 1])

            @pl.when(k < 5)
            def _():
                first(r, p, 1, hid.at[k])

            @pl.when(k == 5)
            def _():
                first(r, p, 1, spare)

        @pl.when(jnp.logical_not(is_first))
        def _():
            @pl.when(k < 5)
            def _():
                second(r, p, 1, hid.at[k], t)

            @pl.when(k == 5)
            def _():
                second(r, p, 1, spare, t)

            for i in range(2):
                m = 2 * p + i
                span = pl.ds(pl.multiple_of(t * tile_out, tile_out), tile_out)
                remote(xs.at[r, m, :, span], back.at[3, m, :, span], r_send.at[r, m], b_recv.at[3, m], device(m, slab)).start()

    def job(j, carry):
        g = jnp.where(inner, j // PAIRS, 3 * (j // PAIRS))
        start = j % PAIRS == 0
        p = jnp.where(g == 4, 1 - j % PAIRS, j % PAIRS)

        @pl.when((g == 0) & start)
        def _():
            for copy in load_a:
                copy.wait()

        @pl.when((g == 1) & start)
        def _():
            for copy in send_c:
                copy.wait_recv()
            load_c[1].start()
            load_b[0].start()
            load_c[0].wait()
            load_c[1].wait()

        @pl.when((g == 3) & start)
        def _():
            @pl.when(inner)
            def _():
                for t in range(tiles):
                    send_b[t].wait_recv()
                    send_do[t].start()

            @pl.when(outer)
            def _():
                forward(1, 0).start()
                for m in order:
                    pass_on(1, m)
                for copy in send_b:
                    copy.wait_recv()
                load_b[0].start()

            load_b[1].start()
            load_b[0].wait()
            load_b[1].wait()

        @pl.when((g == 4) & start)
        def _():
            send_di.wait_recv()
            load_di.start()
            load_di.wait()
            each(0, 24, late_step)

        r = jnp.where(g == 4, 5, g)
        b = jnp.where((g == 0) | (g == 3), 0, 1)
        q = jnp.where(g == 0, 0, jnp.where(g == 3, 1, jnp.where(g == 4, 3, 2)))
        whole(r, q, p, b, g == 2)
        return carry

    lax.fori_loop(0, jnp.where(inner, 4 * PAIRS + 2, 2 * PAIRS), job, 0)

    for q in range(4):
        each(0, 8, lambda m: landed(b_recv.at[q, m]))
        each(1, 8, lambda m: landed(x_send.at[q, m]))
    for r in (0, 3):
        each(1, 8, lambda m: landed(r_send.at[r, m]))
    for copy in send_b:
        copy.wait_send()

    @pl.when(inner)
    def _():
        for r in (1, 2, 4, 5):
            each(0 if r in (2, 4) else 1, 8, lambda m: landed(r_send.at[r, m]))
        for copy in send_c + [send_di] + send_do:
            copy.wait_send()

    @pl.when(outer)
    def _():
        for k in range(2):
            each(0, 8, lambda m: landed(relay_send.at[k, m]))


def exchange(disp, w_in, w_out, wb_in, wc_in):
    _, _, cap, dim = disp.shape
    hidden = w_in.shape[2]
    anywhere = pl.BlockSpec(memory_space=pl.ANY)
    dma = pltpu.SemaphoreType.DMA
    bf16 = jnp.bfloat16
    tile = 256
    in_shape, out_shape = (dim, hidden), (dim // tile, hidden, tile)
    outs = [disp.shape, out_shape, out_shape, in_shape, out_shape, (2,) + disp.shape[1:]]
    return pl.pallas_call(
        exchange_body,
        in_specs=[anywhere] * 5,
        out_specs=[anywhere] * len(outs),
        out_shape=[jax.ShapeDtypeStruct(s, bf16) for s in outs],
        scratch_shapes=[
            pltpu.VMEM((6, 8, cap, dim), bf16),
            pltpu.VMEM((2,) + in_shape, bf16),
            pltpu.VMEM((2,) + out_shape, bf16),
            pltpu.VMEM((PAIRS + 1, 2 * cap, hidden), bf16),
            dma((4, 8)), dma((6, 8)), dma((10,)), dma((10,)), dma((6, 8)), dma((4, 8)), dma((8,)), dma((2, 8)), dma((2, 8)),
        ],
        compiler_params=pltpu.CompilerParams(collective_id=0, has_side_effects=True, vmem_limit_bytes=67043328),
        cost_estimate=pl.CostEstimate(flops=4 * 48 * cap * dim * hidden, bytes_accessed=100 << 20, transcendentals=0),
        name="exchange",
    )(disp, w_in, w_out, wb_in, wc_in)[0]


def lin(x, z, y, c):
    return x * 16 + z * 4 + y * 2 + c


DEVICES = [(x, z, y, c) for x in range(2) for z in range(4) for y in range(2) for c in range(2)]


def solution(mesh):
    swap_near = [(lin(x, z, y, c), lin(x, z ^ 1, y, c)) for x, z, y, c in DEVICES]
    swap_mid = [(lin(x, z, y, c), lin(x, 3 - z, y, c)) for x, z, y, c in DEVICES if z in (1, 2)]

    def local_block(tokens, expert_idx, w_router, w_in, w_out):
        tok_count, dim = tokens.shape
        num_experts = w_router.shape[1]
        capacity = (5 * tok_count + 4 * num_experts - 1) // (4 * num_experts)
        x = lax.axis_index("dp")
        ep = lax.axis_index("ep")
        z, y, c = ep // 4, (ep // 2) % 2, ep % 2

        wa_in = lax.dynamic_index_in_dim(w_in, x, 0, False)
        with jax.named_scope("weights_mid"):
            wc_in = lax.ppermute(wa_in, AXES, swap_mid)
        with jax.named_scope("weights_near"):
            wb_in = lax.ppermute(wa_in, AXES, swap_near)

        logits = jnp.dot(tokens.astype(jnp.float32), w_router, precision=lax.Precision.HIGHEST)
        router_prob = jax.nn.softmax(logits, axis=-1)
        chosen = expert_idx[:, None] == jnp.arange(num_experts, dtype=jnp.int32)[None, :]
        gate = jnp.sum(jnp.where(chosen, router_prob, 0.0), axis=-1)
        running = jnp.cumsum(chosen.astype(jnp.int32), axis=0) - 1
        position = jnp.sum(jnp.where(chosen, running, 0), axis=-1)

        bit_x, bit_c, bit_y, slab = expert_idx & 1, (expert_idx >> 1) & 1, (expert_idx >> 2) & 1, expert_idx >> 3
        mask = ((bit_x ^ x) << 2) | ((bit_y ^ y) << 1) | (bit_c ^ c)
        far = (slab >> 1) != (z >> 1)
        second = jnp.where(far, (slab == 0) | (slab == 3), slab != z)
        block = far.astype(jnp.int32) * 16 + second.astype(jnp.int32) * 8 + mask
        kept = position < capacity
        slot = jnp.where(kept, block * capacity + position, num_experts * capacity)
        holder = jnp.zeros((num_experts * capacity + 1,), jnp.int32).at[slot].set(jnp.arange(tok_count, dtype=jnp.int32))
        disp = jnp.take(tokens, holder[:-1], axis=0, mode="clip").reshape(4, 8, capacity, dim)

        back = exchange(disp, w_in, w_out, wb_in, wc_in)

        picked = jnp.take(back.reshape(num_experts * capacity, dim), jnp.where(kept, slot, 0), axis=0, mode="clip")
        scaled = (gate[:, None] * picked.astype(jnp.float32)).astype(jnp.bfloat16)
        return jnp.where(kept[:, None], scaled, jnp.zeros_like(scaled))

    return jax.shard_map(local_block, mesh=mesh, in_specs=(P(AXES, None), P(AXES), P(None, None), P("ep", None, None), P("ep", None, None)), out_specs=P(AXES, None), check_vma=False)
```

```python
import jax
import jax.numpy as jnp
from jax import lax
from jax.experimental import pallas as pl
from jax.experimental.pallas import tpu as pltpu
from jax.sharding import PartitionSpec as P

AXES = ("dp", "ep")
MESH = pl.DeviceIdType.MESH
PAIRS = 4


def exchange_body(disp, w_in, w_out, wb_in, wc_in, router,
                  back, wb_out, wc_out, wd_in, wd_out, relay,
                  xs, wi, wo, hid, gates, nothing, x_send, x_recv, w_send, w_recv, r_send, b_recv, w_load, relay_recv, relay_send, zero_sem):
    x = lax.axis_index("dp")
    ep = lax.axis_index("ep")
    z, y, c = ep // 4, (ep // 2) % 2, ep % 2
    inner = (z == 1) | (z == 2)
    outer = jnp.logical_not(inner)
    z_near = z + 1 - 2 * (z % 2)
    z_mid = 3 - z
    cap, dim = xs.shape[2:]
    hidden = wi.shape[2]
    tiles, tile_out = wo.shape[1], wo.shape[3]
    rows = 2 * cap
    tile_in = 512

    def device(m, slab):
        return ((x + m // 4) % 2, slab * 4 + ((y + (m // 2) % 2) % 2) * 2 + (c + m % 2) % 2)

    def remote(src, dst, send, recv, dev):
        return pltpu.make_async_remote_copy(src, dst, send, recv, device_id=dev, device_id_type=MESH)

    barrier = pltpu.get_barrier_semaphore()
    for m in range(1, 8):
        pl.semaphore_signal(barrier, inc=1, device_id=device(m, z), device_id_type=MESH)
    for m in range(8):
        pl.semaphore_signal(barrier, inc=1, device_id=device(m, z_near), device_id_type=MESH)
    pl.semaphore_signal(barrier, inc=1, device_id=device(0, z_mid), device_id_type=MESH)
    pl.semaphore_wait(barrier, 16)

    def cols(t):
        return pl.ds(t * tile_out, tile_out)

    def weight(src, dst, k, slab):
        return remote(src, dst, w_send.at[k], w_recv.at[k], device(0, slab))

    send_b = [weight(w_out.at[x, :, cols(t)], wb_out.at[t], t, z_near) for t in range(tiles)]
    send_c = [weight(w_out.at[x, :, cols(t)], wc_out.at[t], 3 + t, z_mid) for t in range(tiles)]
    send_di = weight(wb_in, wd_in, 6, z_mid)
    send_do = [weight(wb_out.at[t], wd_out.at[t], 7 + t, z_mid) for t in range(tiles)]

    def load(src, dst, k):
        return pltpu.make_async_copy(src, dst, w_load.at[k])

    load_a = [load(w_in.at[x], wi.at[0], 0)] + [load(w_out.at[x, :, cols(t)], wo.at[0, t], 1 + t) for t in range(tiles)]
    load_b = [load(wb_in, wi.at[0], 0), load(wb_out, wo.at[0], 1)]
    load_c = [load(wc_in, wi.at[1], 4), load(wc_out, wo.at[1], 5)]
    load_di = load(wd_in, wi.at[1], 4)
    load_do = [load(wd_out.at[t], wo.at[1, t], 5 + t) for t in range(tiles)]

    def landed(sem):
        pltpu.make_async_copy(xs.at[0, 0], xs.at[0, 0], sem).wait()

    def home(q, m):
        return back.at[q * 8 + m]

    nothing[...] = jnp.zeros_like(nothing)
    gates[...] = jnp.zeros_like(gates)
    clear = pltpu.make_async_copy(nothing, back.at[32, pl.ds(0, nothing.shape[0])], zero_sem)
    clear.start()

    def own(q, r):
        return pltpu.make_async_copy(disp.at[q, 0], xs.at[r, 0], x_recv.at[r, 0])

    def dispatch(q, r, m, slab):
        return remote(disp.at[q, m], xs.at[r, m], x_send.at[q, m], x_recv.at[r, m], device(m, slab))

    @pl.when(inner)
    def _():
        for copy in send_b + send_c + [send_di]:
            copy.start()

    def hand(k, m):
        return remote(disp.at[2 + k, m], relay.at[k, m], x_send.at[2 + k, m], relay_recv.at[k, m], device(m, z))

    def forward(k, m):
        src = relay.at[k, m] if m else disp.at[2 + k, 0]
        return remote(src, xs.at[2 + 2 * k, m], relay_send.at[k, m], x_recv.at[2 + 2 * k, m], device(0, z_near))

    order = (1, 2, 4, 3, 5, 6, 7)

    @pl.when(outer)
    def _():
        for m in order:
            hand(0, m).start()
        forward(0, 0).start()
        send_b[0].start()

    own(0, 0).start()
    own(1, 3).start()
    for copy in load_a:
        copy.start()

    for m in order:
        dispatch(0, 0, m, z).start()

    @pl.when(inner)
    def _():
        load_c[0].start()
        own(2, 1).start()
        own(3, 5).start()
        for m in order:
            dispatch(2, 1, m, z).start()

    @pl.when(outer)
    def _():
        for m in order:
            hand(1, m).start()

    for m in order:
        dispatch(1, 3, m, z).start()

    @pl.when(inner)
    def _():
        for m in order:
            dispatch(3, 5, m, z).start()

    def pass_on(k, m):
        landed(relay_recv.at[k, m])
        forward(k, m).start()

    @pl.when(outer)
    def _():
        for m in order:
            pass_on(0, m)
        send_b[1].start()
        send_b[2].start()

    def first(r, p, b, kept):
        view = xs.at[r]

        def step(n, carry):
            span = pl.ds(pl.multiple_of(n * tile_in, tile_in), tile_in)
            value = jnp.dot(view[pl.ds(2 * p, 2)].reshape(rows, dim), wi[b, :, span], preferred_element_type=jnp.float32)
            kept[:, span] = jnp.maximum(value, 0.0).astype(jnp.bfloat16)
            return carry

        lax.fori_loop(0, hidden // tile_in, step, 0)

    def gate(r, p, k):
        part = xs[r, pl.ds(2 * p, 2)].reshape(rows, dim)
        logits = jnp.dot(part, router[2], preferred_element_type=jnp.float32)
        logits = logits + jnp.dot(part, router[1], preferred_element_type=jnp.float32)
        logits = logits + jnp.dot(part, router[0], preferred_element_type=jnp.float32)
        lane = lax.broadcasted_iota(jnp.int32, logits.shape, 1)
        slab = jnp.where(r == 0, z, jnp.where(r == 3, z_near, jnp.where(r < 3, z_mid, 3 - z_near)))
        expert = slab * 8 + y * 4 + c * 2 + x
        logits = jnp.where(lane < 32, logits, -jnp.inf)
        weight = jnp.exp(logits - jnp.max(logits, axis=1, keepdims=True))
        chosen = jnp.sum(jnp.where(lane == expert, weight, 0.0), axis=1, keepdims=True)
        gates[...] = jnp.where(lane == k, chosen / jnp.sum(weight, axis=1, keepdims=True), gates[...])

    def second(r, p, b, kept, k, t):
        value = jnp.dot(kept[...], wo[b, t], preferred_element_type=jnp.float32)
        lane = lax.broadcasted_iota(jnp.int32, gates.shape, 1)
        scale = jnp.sum(jnp.where(lane == k, gates[...], 0.0), axis=1, keepdims=True)
        value = scale * value.astype(jnp.bfloat16).astype(jnp.float32)
        span = pl.ds(pl.multiple_of(t * tile_out, tile_out), tile_out)
        xs[r, pl.ds(2 * p, 2), :, span] = value.astype(jnp.bfloat16).reshape(2, cap, tile_out)

    def each(lo, hi, fn):
        def step(i, carry):
            fn(i)
            return carry

        lax.fori_loop(lo, hi, step, 0)

    def send_back(r, q, p, edge):
        slab = jnp.where(edge, z_near, z)

        def result(m):
            return remote(xs.at[r, m], home(q, m), r_send.at[r, m], b_recv.at[q, m], device(m, slab))

        keep = (p == 0) & jnp.logical_not(edge)

        @pl.when(keep)
        def _():
            pltpu.make_async_copy(xs.at[r, 0], home(q, 0), b_recv.at[q, 0]).start()

        @pl.when(jnp.logical_not(keep))
        def _():
            result(2 * p).start()

        result(2 * p + 1).start()

    def whole(r, q, p, b, edge):
        landed(x_recv.at[r, 2 * p])
        landed(x_recv.at[r, 2 * p + 1])
        gate(r, p, 0)
        first(r, p, b, hid.at[0])
        each(0, tiles, lambda t: second(r, p, b, hid.at[0], 0, t))
        send_back(r, q, p, edge)

    def late_step(s):
        is_first = (s < 4) | (s == 8) | (s == 13)
        k = jnp.where(s < 2, 4 + s, jnp.where(s < 6, s % 2, jnp.where(s < 8, s - 2, jnp.where(s < 10, 2, jnp.where(s < 13, s - 10, jnp.where(s < 16, 3, jnp.where(s < 18, s - 12, s % 6)))))))
        t = jnp.where((s < 10) | (s == 14), 0, jnp.where(s < 18, 1, 2))
        edge = k < 4
        r = jnp.where(edge, 4, 5)
        p = jnp.where(edge, k, 7 - k)
        slab = jnp.where(edge, z_near, z)
        spare = wi.at[0, pl.ds(0, rows)]

        for step, tile in ((4, 0), (10, 1), (18, 2)):
            @pl.when(s == step)
            def _():
                send_do[tile].wait_recv()
                load_do[tile].start()
                load_do[tile].wait()

        @pl.when(is_first)
        def _():
            landed(x_recv.at[r, 2 * p])
            landed(x_recv.at[r, 2 * p + 1])
            gate(r, p, k)

            @pl.when(k < 5)
            def _():
                first(r, p, 1, hid.at[k])

            @pl.when(k == 5)
            def _():
                first(r, p, 1, spare)

        @pl.when(jnp.logical_not(is_first))
        def _():
            @pl.when(k < 5)
            def _():
                second(r, p, 1, hid.at[k], k, t)

            @pl.when(k == 5)
            def _():
                second(r, p, 1, spare, 5, t)

            for i in range(2):
                m = 2 * p + i
                span = pl.ds(pl.multiple_of(t * tile_out, tile_out), tile_out)
                remote(xs.at[r, m, :, span], home(3, m).at[:, span], r_send.at[r, m], b_recv.at[3, m], device(m, slab)).start()

    def job(j, carry):
        g = jnp.where(inner, j // PAIRS, 3 * (j // PAIRS))
        start = j % PAIRS == 0
        p = jnp.where(g == 4, 1 - j % PAIRS, j % PAIRS)

        @pl.when((g == 0) & start)
        def _():
            for copy in load_a:
                copy.wait()

        @pl.when((g == 1) & start)
        def _():
            for copy in send_c:
                copy.wait_recv()
            load_c[1].start()
            load_b[0].start()
            load_c[0].wait()
            load_c[1].wait()

        @pl.when((g == 3) & start)
        def _():
            @pl.when(inner)
            def _():
                for t in range(tiles):
                    send_b[t].wait_recv()
                    send_do[t].start()

            @pl.when(outer)
            def _():
                forward(1, 0).start()
                for m in order:
                    pass_on(1, m)
                for copy in send_b:
                    copy.wait_recv()
                load_b[0].start()

            load_b[1].start()
            load_b[0].wait()
            load_b[1].wait()

        @pl.when((g == 4) & start)
        def _():
            send_di.wait_recv()
            load_di.start()
            load_di.wait()
            each(0, 24, late_step)

        r = jnp.where(g == 4, 5, g)
        b = jnp.where((g == 0) | (g == 3), 0, 1)
        q = jnp.where(g == 0, 0, jnp.where(g == 3, 1, jnp.where(g == 4, 3, 2)))
        whole(r, q, p, b, g == 2)
        return carry

    lax.fori_loop(0, jnp.where(inner, 4 * PAIRS + 2, 2 * PAIRS), job, 0)

    for q in range(4):
        each(0, 8, lambda m: landed(b_recv.at[q, m]))
        each(1, 8, lambda m: landed(x_send.at[q, m]))
    for r in (0, 3):
        each(1, 8, lambda m: landed(r_send.at[r, m]))
    clear.wait()
    for copy in send_b:
        copy.wait_send()

    @pl.when(inner)
    def _():
        for r in (1, 2, 4, 5):
            each(0 if r in (2, 4) else 1, 8, lambda m: landed(r_send.at[r, m]))
        for copy in send_c + [send_di] + send_do:
            copy.wait_send()

    @pl.when(outer)
    def _():
        for k in range(2):
            each(0, 8, lambda m: landed(relay_send.at[k, m]))


def exchange(disp, w_in, w_out, wb_in, wc_in, router):
    _, _, cap, dim = disp.shape
    hidden = w_in.shape[2]
    anywhere = pl.BlockSpec(memory_space=pl.ANY)
    dma = pltpu.SemaphoreType.DMA
    bf16 = jnp.bfloat16
    tile = 256
    in_shape, out_shape = (dim, hidden), (dim // tile, hidden, tile)
    outs = [(33, cap, dim), out_shape, out_shape, in_shape, out_shape, (2,) + disp.shape[1:]]
    return pl.pallas_call(
        exchange_body,
        in_specs=[anywhere] * 5 + [pl.BlockSpec(memory_space=pltpu.VMEM)],
        out_specs=[anywhere] * len(outs),
        out_shape=[jax.ShapeDtypeStruct(s, bf16) for s in outs],
        scratch_shapes=[
            pltpu.VMEM((6, 8, cap, dim), bf16),
            pltpu.VMEM((2,) + in_shape, bf16),
            pltpu.VMEM((2,) + out_shape, bf16),
            pltpu.VMEM((PAIRS + 1, 2 * cap, hidden), bf16),
            pltpu.VMEM((2 * cap, 128), jnp.float32),
            pltpu.VMEM((16, dim), bf16),
            dma((4, 8)), dma((6, 8)), dma((10,)), dma((10,)), dma((6, 8)), dma((4, 8)), dma((8,)), dma((2, 8)), dma((2, 8)), dma,
        ],
        compiler_params=pltpu.CompilerParams(collective_id=0, has_side_effects=True, vmem_limit_bytes=67043328),
        cost_estimate=pl.CostEstimate(flops=4 * 48 * cap * dim * hidden, bytes_accessed=100 << 20, transcendentals=0),
        name="exchange",
    )(disp, w_in, w_out, wb_in, wc_in, router)[0]


def lin(x, z, y, c):
    return x * 16 + z * 4 + y * 2 + c


DEVICES = [(x, z, y, c) for x in range(2) for z in range(4) for y in range(2) for c in range(2)]


def solution(mesh):
    swap_near = [(lin(x, z, y, c), lin(x, z ^ 1, y, c)) for x, z, y, c in DEVICES]
    swap_mid = [(lin(x, z, y, c), lin(x, 3 - z, y, c)) for x, z, y, c in DEVICES if z in (1, 2)]

    def local_block(tokens, expert_idx, w_router, w_in, w_out):
        tok_count, dim = tokens.shape
        num_experts = w_router.shape[1]
        capacity = (5 * tok_count + 4 * num_experts - 1) // (4 * num_experts)
        x = lax.axis_index("dp")
        ep = lax.axis_index("ep")
        z, y, c = ep // 4, (ep // 2) % 2, ep % 2

        wa_in = lax.dynamic_index_in_dim(w_in, x, 0, False)
        with jax.named_scope("weights_mid"):
            wc_in = lax.ppermute(wa_in, AXES, swap_mid)
        with jax.named_scope("weights_near"):
            wb_in = lax.ppermute(wa_in, AXES, swap_near)

        high = lax.reduce_precision(w_router, 8, 7)
        middle = lax.reduce_precision(w_router - high, 8, 7)
        low = (w_router - high) - middle
        router = jnp.stack([high, middle, low]).astype(jnp.bfloat16)
        router = jnp.pad(router, ((0, 0), (0, 0), (0, 128 - num_experts)))

        chosen = expert_idx[:, None] == jnp.arange(num_experts, dtype=jnp.int32)[None, :]
        running = jnp.cumsum(chosen.astype(jnp.int32), axis=0) - 1
        position = jnp.sum(jnp.where(chosen, running, 0), axis=-1)

        bit_x, bit_c, bit_y, slab = expert_idx & 1, (expert_idx >> 1) & 1, (expert_idx >> 2) & 1, expert_idx >> 3
        mask = ((bit_x ^ x) << 2) | ((bit_y ^ y) << 1) | (bit_c ^ c)
        far = (slab >> 1) != (z >> 1)
        second = jnp.where(far, (slab == 0) | (slab == 3), slab != z)
        block = far.astype(jnp.int32) * 16 + second.astype(jnp.int32) * 8 + mask
        kept = position < capacity
        slot = jnp.where(kept, block * capacity + position, num_experts * capacity)
        holder = jnp.zeros((num_experts * capacity + 1,), jnp.int32).at[slot].set(jnp.arange(tok_count, dtype=jnp.int32))
        disp = jnp.take(tokens, holder[:-1], axis=0, mode="clip").reshape(4, 8, capacity, dim)

        back = exchange(disp, w_in, w_out, wb_in, wc_in, router).reshape(-1, dim)

        return jnp.take(back, slot, axis=0, mode="clip")

    return jax.shard_map(local_block, mesh=mesh, in_specs=(P(AXES, None), P(AXES), P(None, None), P("ep", None, None), P("ep", None, None)), out_specs=P(AXES, None), check_vma=False)
```

```python
import jax
import jax.numpy as jnp
from jax import lax
from jax.experimental import pallas as pl
from jax.experimental.pallas import tpu as pltpu
from jax.sharding import PartitionSpec as P

AXES = ("dp", "ep")
MESH = pl.DeviceIdType.MESH
PAIRS = 4


def exchange_body(disp, w_in, w_out, wb_in, wc_in, router,
                  back, wb_out, wc_out, wd_in, wd_out, relay, wb_rest, wc_rest, wd_rest,
                  xs, wi, wo, hid, gates, nothing, x_send, x_recv, w_send, w_recv, r_send, b_recv, w_load, relay_recv, relay_send, zero_sem):
    x = lax.axis_index("dp")
    ep = lax.axis_index("ep")
    z, y, c = ep // 4, (ep // 2) % 2, ep % 2
    inner = (z == 1) | (z == 2)
    outer = jnp.logical_not(inner)
    z_near = z + 1 - 2 * (z % 2)
    z_mid = 3 - z
    cap, dim = xs.shape[2:]
    hidden = wi.shape[2]
    tiles, tile_out = wo.shape[1], wo.shape[3]
    rows = 2 * cap
    tile_in = 512

    def device(m, slab):
        return ((x + m // 4) % 2, slab * 4 + ((y + (m // 2) % 2) % 2) * 2 + (c + m % 2) % 2)

    def remote(src, dst, send, recv, dev):
        return pltpu.make_async_remote_copy(src, dst, send, recv, device_id=dev, device_id_type=MESH)

    barrier = pltpu.get_barrier_semaphore()
    for m in range(1, 8):
        pl.semaphore_signal(barrier, inc=1, device_id=device(m, z), device_id_type=MESH)
    for m in range(8):
        pl.semaphore_signal(barrier, inc=1, device_id=device(m, z_near), device_id_type=MESH)
    pl.semaphore_signal(barrier, inc=1, device_id=device(0, z_mid), device_id_type=MESH)
    pl.semaphore_wait(barrier, 16)

    def cols(t):
        return pl.ds(t * tile_out, tile_out)

    split = wb_in.shape[1]
    most, rest = pl.ds(0, split), pl.ds(split, hidden - split)

    def weight(src, dst, k, slab):
        return remote(src, dst, w_send.at[k], w_recv.at[k], device(0, slab))

    send_b = [weight(w_out.at[x, :, cols(t)], wb_out.at[t], t, z_near) for t in range(tiles)]
    send_c = [weight(w_out.at[x, :, cols(t)], wc_out.at[t], 3 + t, z_mid) for t in range(tiles)]
    send_di = weight(wb_in, wd_in, 6, z_mid)
    send_do = [weight(wb_out.at[t], wd_out.at[t], 7 + t, z_mid) for t in range(tiles)]

    send_br = weight(w_in.at[x, :, rest], wb_rest, 10, z_near)
    send_cr = weight(w_in.at[x, :, rest], wc_rest, 11, z_mid)
    send_dr = weight(wb_rest, wd_rest, 12, z_mid)

    def load(src, dst, k):
        return pltpu.make_async_copy(src, dst, w_load.at[k])

    load_a = [load(w_in.at[x], wi.at[0], 0)] + [load(w_out.at[x, :, cols(t)], wo.at[0, t], 1 + t) for t in range(tiles)]
    load_b = [load(wb_in, wi.at[0, :, most], 0), load(wb_out, wo.at[0], 1), load(wb_rest, wi.at[0, :, rest], 8)]
    load_c = [load(wc_in, wi.at[1, :, most], 4), load(wc_out, wo.at[1], 5), load(wc_rest, wi.at[1, :, rest], 9)]
    load_di = load(wd_in, wi.at[1, :, most], 4)
    load_dr = load(wd_rest, wi.at[1, :, rest], 10)
    load_do = [load(wd_out.at[t], wo.at[1, t], 5 + t) for t in range(tiles)]

    def landed(sem):
        pltpu.make_async_copy(xs.at[0, 0], xs.at[0, 0], sem).wait()

    def home(q, m):
        return back.at[q * 8 + m]

    nothing[...] = jnp.zeros_like(nothing)
    gates[...] = jnp.zeros_like(gates)
    clear = pltpu.make_async_copy(nothing, back.at[32, pl.ds(0, nothing.shape[0])], zero_sem)
    clear.start()

    def own(q, r):
        return pltpu.make_async_copy(disp.at[q, 0], xs.at[r, 0], x_recv.at[r, 0])

    def dispatch(q, r, m, slab):
        return remote(disp.at[q, m], xs.at[r, m], x_send.at[q, m], x_recv.at[r, m], device(m, slab))

    @pl.when(inner)
    def _():
        for copy in [send_br] + send_b + [send_cr] + send_c + [send_di]:
            copy.start()

    def hand(k, m):
        return remote(disp.at[2 + k, m], relay.at[k, m], x_send.at[2 + k, m], relay_recv.at[k, m], device(m, z))

    def forward(k, m):
        src = relay.at[k, m] if m else disp.at[2 + k, 0]
        return remote(src, xs.at[2 + 2 * k, m], relay_send.at[k, m], x_recv.at[2 + 2 * k, m], device(0, z_near))

    order = (1, 2, 4, 3, 5, 6, 7)

    @pl.when(outer)
    def _():
        for m in order:
            hand(0, m).start()
        forward(0, 0).start()
        send_b[0].start()

    own(0, 0).start()
    own(1, 3).start()
    for copy in load_a:
        copy.start()

    for m in order:
        dispatch(0, 0, m, z).start()

    @pl.when(inner)
    def _():
        load_c[0].start()
        own(2, 1).start()
        own(3, 5).start()
        for m in order:
            dispatch(2, 1, m, z).start()

    @pl.when(outer)
    def _():
        for m in order:
            hand(1, m).start()

    for m in order:
        dispatch(1, 3, m, z).start()

    @pl.when(inner)
    def _():
        for m in order:
            dispatch(3, 5, m, z).start()

    def pass_on(k, m):
        landed(relay_recv.at[k, m])
        forward(k, m).start()

    @pl.when(outer)
    def _():
        for m in order:
            pass_on(0, m)
        send_br.start()
        send_b[1].start()
        send_b[2].start()

    def first(r, p, b, kept):
        view = xs.at[r]

        def step(n, carry):
            span = pl.ds(pl.multiple_of(n * tile_in, tile_in), tile_in)
            value = jnp.dot(view[pl.ds(2 * p, 2)].reshape(rows, dim), wi[b, :, span], preferred_element_type=jnp.float32)
            kept[:, span] = jnp.maximum(value, 0.0).astype(jnp.bfloat16)
            return carry

        lax.fori_loop(0, hidden // tile_in, step, 0)

    def gate(r, p, k):
        part = xs[r, pl.ds(2 * p, 2)].reshape(rows, dim)
        logits = jnp.dot(part, router[2], preferred_element_type=jnp.float32)
        logits = logits + jnp.dot(part, router[1], preferred_element_type=jnp.float32)
        logits = logits + jnp.dot(part, router[0], preferred_element_type=jnp.float32)
        lane = lax.broadcasted_iota(jnp.int32, logits.shape, 1)
        slab = jnp.where(r == 0, z, jnp.where(r == 3, z_near, jnp.where(r < 3, z_mid, 3 - z_near)))
        expert = slab * 8 + y * 4 + c * 2 + x
        logits = jnp.where(lane < 32, logits, -jnp.inf)
        weight = jnp.exp(logits - jnp.max(logits, axis=1, keepdims=True))
        chosen = jnp.sum(jnp.where(lane == expert, weight, 0.0), axis=1, keepdims=True)
        gates[...] = jnp.where(lane == k, chosen / jnp.sum(weight, axis=1, keepdims=True), gates[...])

    def finish(r, p, k, t, value):
        lane = lax.broadcasted_iota(jnp.int32, gates.shape, 1)
        scale = jnp.sum(jnp.where(lane == k, gates[...], 0.0), axis=1, keepdims=True)
        value = scale * value.astype(jnp.bfloat16).astype(jnp.float32)
        span = pl.ds(pl.multiple_of(t * tile_out, tile_out), tile_out)
        xs[r, pl.ds(2 * p, 2), :, span] = value.astype(jnp.bfloat16).reshape(2, cap, tile_out)

    def second(r, p, b, kept, k, t):
        finish(r, p, k, t, jnp.dot(kept[...], wo[b, t], preferred_element_type=jnp.float32))

    blocks = hidden // dim

    def first_split(r, p, region):
        def step(i, carry):
            span = pl.ds(pl.multiple_of(i * tile_out, tile_out), tile_out)
            place = pl.ds(pl.multiple_of(i % tiles * tile_out, tile_out), tile_out)
            value = jnp.dot(xs[r, pl.ds(2 * p, 2)].reshape(rows, dim), wi[1, :, span], preferred_element_type=jnp.float32)
            value = jnp.maximum(value, 0.0).astype(jnp.bfloat16)
            xs[region, pl.ds(2 * (i // tiles), 2), :, place] = value.reshape(2, cap, tile_out)
            return carry

        lax.fori_loop(0, hidden // tile_out, step, 0)

    def second_split(r, p, region, k, t):
        value = None
        for n in range(blocks):
            part = xs[region, pl.ds(2 * n, 2)].reshape(rows, dim)
            term = jnp.dot(part, wo[1, t, pl.ds(n * dim, dim), :], preferred_element_type=jnp.float32)
            value = term if value is None else value + term
        finish(r, p, k, t, value)

    def each(lo, hi, fn):
        def step(i, carry):
            fn(i)
            return carry

        lax.fori_loop(lo, hi, step, 0)

    def send_back(r, q, p, edge):
        slab = jnp.where(edge, z_near, z)

        def result(m):
            return remote(xs.at[r, m], home(q, m), r_send.at[r, m], b_recv.at[q, m], device(m, slab))

        keep = (p == 0) & jnp.logical_not(edge)

        @pl.when(keep)
        def _():
            pltpu.make_async_copy(xs.at[r, 0], home(q, 0), b_recv.at[q, 0]).start()

        @pl.when(jnp.logical_not(keep))
        def _():
            result(2 * p).start()

        result(2 * p + 1).start()

    def whole(r, q, p, b, edge):
        landed(x_recv.at[r, 2 * p])
        landed(x_recv.at[r, 2 * p + 1])
        gate(r, p, 0)
        first(r, p, b, hid.at[0])
        each(0, tiles, lambda t: second(r, p, b, hid.at[0], 0, t))
        send_back(r, q, p, edge)

    def late_step(s):
        is_first = (s < 2) | (s == 4) | (s == 5) | (s == 7) | (s == 11) | (s == 18) | (s == 19)
        k = jnp.where(s == 4, 4, jnp.where(s == 7, 5, jnp.where(s < 4, s % 2, jnp.where(s < 7, 2, s - 8))))
        k = jnp.where(s < 11, k, jnp.where(s < 14, 3, jnp.where(s < 18, 4 + s % 2, jnp.where(s < 24, 6 + s % 2, jnp.where(s < 28, 27 - s, s - 24)))))
        early = (s < 8) | (s == 12) | (s == 14) | (s == 15) | (s == 20) | (s == 21)
        t = jnp.where(early, 0, jnp.where(s < 24, 1, 2))
        edge = k < 4
        r = jnp.where(edge, 4, 5)
        p = jnp.where(edge, k, 7 - k)
        slab = jnp.where(edge, z_near, z)
        spare = wi.at[0, pl.ds(0, rows)]

        @pl.when(s == 18)
        def _():
            for q, region in ((0, 0), (2, 1)):
                landed(b_recv.at[q, 0])
                each(1, 8, lambda m: landed(r_send.at[region, m]))

        for step, tile in ((2, 0), (8, 1), (24, 2)):
            @pl.when(s == step)
            def _():
                send_do[tile].wait_recv()
                load_do[tile].start()
                load_do[tile].wait()

        @pl.when(is_first)
        def _():
            landed(x_recv.at[r, 2 * p])
            landed(x_recv.at[r, 2 * p + 1])
            gate(r, p, k)

            @pl.when(k < 5)
            def _():
                first(r, p, 1, hid.at[k])

            @pl.when(k == 5)
            def _():
                first(r, p, 1, spare)

            @pl.when(k > 5)
            def _():
                first_split(r, p, k - 6)

        @pl.when(jnp.logical_not(is_first))
        def _():
            @pl.when(k < 5)
            def _():
                second(r, p, 1, hid.at[k], k, t)

            @pl.when(k == 5)
            def _():
                second(r, p, 1, spare, 5, t)

            @pl.when(k > 5)
            def _():
                second_split(r, p, k - 6, k, t)

            span = pl.ds(pl.multiple_of(t * tile_out, tile_out), tile_out)

            def tile_back(m):
                return remote(xs.at[r, m, :, span], home(3, m).at[:, span], r_send.at[r, m], b_recv.at[3, m], device(m, slab))

            @pl.when(k == 7)
            def _():
                pltpu.make_async_copy(xs.at[5, 0, :, span], home(3, 0).at[:, span], b_recv.at[3, 0]).start()

            @pl.when(k != 7)
            def _():
                tile_back(2 * p).start()

            tile_back(2 * p + 1).start()

    def job(j, carry):
        g = jnp.where(inner, j // PAIRS, 3 * (j // PAIRS))
        p = j % PAIRS
        start = p == 0

        @pl.when((g == 0) & start)
        def _():
            for copy in load_a:
                copy.wait()

        @pl.when((g == 1) & start)
        def _():
            for copy in [send_cr] + send_c:
                copy.wait_recv()
            load_c[1].start()
            load_c[2].start()
            load_b[0].start()
            for copy in load_c:
                copy.wait()

        @pl.when((g == 3) & start)
        def _():
            @pl.when(inner)
            def _():
                send_br.wait_recv()
                send_dr.start()
                for t in range(tiles):
                    send_b[t].wait_recv()
                    send_do[t].start()

            @pl.when(outer)
            def _():
                forward(1, 0).start()
                for m in range(1, 8):
                    pass_on(1, m)
                for copy in [send_br] + send_b:
                    copy.wait_recv()
                load_b[0].start()

            load_b[1].start()
            load_b[2].start()
            for copy in load_b:
                copy.wait()

        b = jnp.where((g == 0) | (g == 3), 0, 1)
        q = jnp.where(g == 0, 0, jnp.where(g == 3, 1, 2))
        whole(g, q, p, b, g == 2)
        return carry

    lax.fori_loop(0, jnp.where(inner, 4 * PAIRS, 2 * PAIRS), job, 0)

    @pl.when(inner)
    def _():
        send_di.wait_recv()
        load_di.start()
        send_dr.wait_recv()
        load_dr.start()
        load_di.wait()
        load_dr.wait()
        each(0, 32, late_step)

    done = jnp.where(inner, 1, 0)

    for q in range(4):
        each(done if q in (0, 2) else 0, 8, lambda m: landed(b_recv.at[q, m]))
        each(1, 8, lambda m: landed(x_send.at[q, m]))
    each(1, jnp.where(inner, 1, 8), lambda m: landed(r_send.at[0, m]))
    each(1, 8, lambda m: landed(r_send.at[3, m]))
    clear.wait()
    for copy in [send_br] + send_b:
        copy.wait_send()

    @pl.when(inner)
    def _():
        for r in (2, 4, 5):
            each(0 if r in (2, 4) else 1, 8, lambda m: landed(r_send.at[r, m]))
        for copy in [send_cr, send_dr] + send_c + [send_di] + send_do:
            copy.wait_send()

    @pl.when(outer)
    def _():
        for k in range(2):
            each(0, 8, lambda m: landed(relay_send.at[k, m]))


def exchange(disp, w_in, w_out, wb_in, wc_in, router):
    _, _, cap, dim = disp.shape
    hidden = w_in.shape[2]
    anywhere = pl.BlockSpec(memory_space=pl.ANY)
    dma = pltpu.SemaphoreType.DMA
    bf16 = jnp.bfloat16
    tile = 256
    in_shape, out_shape = (dim, hidden), (dim // tile, hidden, tile)
    rest = (dim, hidden - wb_in.shape[1])
    outs = [(33, cap, dim), out_shape, out_shape, wb_in.shape, out_shape, (2,) + disp.shape[1:], rest, rest, rest]
    return pl.pallas_call(
        exchange_body,
        in_specs=[anywhere] * 5 + [pl.BlockSpec(memory_space=pltpu.VMEM)],
        out_specs=[anywhere] * len(outs),
        out_shape=[jax.ShapeDtypeStruct(s, bf16) for s in outs],
        scratch_shapes=[
            pltpu.VMEM((6, 8, cap, dim), bf16),
            pltpu.VMEM((2,) + in_shape, bf16),
            pltpu.VMEM((2,) + out_shape, bf16),
            pltpu.VMEM((PAIRS + 1, 2 * cap, hidden), bf16),
            pltpu.VMEM((2 * cap, 128), jnp.float32),
            pltpu.VMEM((16, dim), bf16),
            dma((4, 8)), dma((6, 8)), dma((13,)), dma((13,)), dma((6, 8)), dma((4, 8)), dma((11,)), dma((2, 8)), dma((2, 8)), dma,
        ],
        compiler_params=pltpu.CompilerParams(collective_id=0, has_side_effects=True, vmem_limit_bytes=67043328),
        cost_estimate=pl.CostEstimate(flops=4 * 48 * cap * dim * hidden, bytes_accessed=100 << 20, transcendentals=0),
        name="exchange",
    )(disp, w_in, w_out, wb_in, wc_in, router)[0]


def lin(x, z, y, c):
    return x * 16 + z * 4 + y * 2 + c


DEVICES = [(x, z, y, c) for x in range(2) for z in range(4) for y in range(2) for c in range(2)]


def solution(mesh):
    swap_near = [(lin(x, z, y, c), lin(x, z ^ 1, y, c)) for x, z, y, c in DEVICES]
    swap_mid = [(lin(x, z, y, c), lin(x, 3 - z, y, c)) for x, z, y, c in DEVICES if z in (1, 2)]

    def local_block(tokens, expert_idx, w_router, w_in, w_out):
        tok_count, dim = tokens.shape
        num_experts = w_router.shape[1]
        capacity = (5 * tok_count + 4 * num_experts - 1) // (4 * num_experts)
        x = lax.axis_index("dp")
        ep = lax.axis_index("ep")
        z, y, c = ep // 4, (ep // 2) % 2, ep % 2

        early = w_in.shape[2] * 5 // 6
        wa_in = lax.dynamic_slice(w_in, (x, 0, 0), (1, dim, early))[0]
        with jax.named_scope("weights_mid"):
            wc_in = lax.ppermute(wa_in, AXES, swap_mid)
        with jax.named_scope("weights_near"):
            wb_in = lax.ppermute(wa_in, AXES, swap_near)

        largest = float(jnp.finfo(jnp.bfloat16).max)
        high = jnp.clip(lax.reduce_precision(w_router, 8, 7), -largest, largest)
        middle = lax.reduce_precision(w_router - high, 8, 7)
        low = (w_router - high) - middle
        router = jnp.stack([high, middle, low]).astype(jnp.bfloat16)
        router = jnp.pad(router, ((0, 0), (0, 0), (0, 128 - num_experts)))

        chosen = expert_idx[:, None] == jnp.arange(num_experts, dtype=jnp.int32)[None, :]
        running = jnp.cumsum(chosen.astype(jnp.int32), axis=0) - 1
        position = jnp.sum(jnp.where(chosen, running, 0), axis=-1)

        bit_x, bit_c, bit_y, slab = expert_idx & 1, (expert_idx >> 1) & 1, (expert_idx >> 2) & 1, expert_idx >> 3
        mask = ((bit_x ^ x) << 2) | ((bit_y ^ y) << 1) | (bit_c ^ c)
        far = (slab >> 1) != (z >> 1)
        second = jnp.where(far, (slab == 0) | (slab == 3), slab != z)
        block = far.astype(jnp.int32) * 16 + second.astype(jnp.int32) * 8 + mask
        kept = position < capacity
        slot = jnp.where(kept, block * capacity + position, num_experts * capacity)
        row_of = block[:, None] == jnp.arange(num_experts, dtype=jnp.int32)[None, :]
        at_position = position[:, None] == jnp.arange(capacity, dtype=jnp.int32)[None, :]
        token = jnp.arange(tok_count, dtype=jnp.int32)
        digits = [jnp.where(at_position, d[:, None], 0).astype(jnp.bfloat16) for d in (token // 128, token % 128)]
        held = [jnp.einsum("te,tp->ep", row_of.astype(jnp.bfloat16), d, preferred_element_type=jnp.float32) for d in digits]
        holder = (held[0] * 128.0 + held[1]).astype(jnp.int32).reshape(num_experts * capacity)
        disp = jnp.take(tokens, holder, axis=0, mode="clip").reshape(4, 8, capacity, dim)

        back = exchange(disp, w_in, w_out, wb_in, wc_in, router).reshape(-1, dim)

        return jnp.take(back, slot, axis=0, mode="clip")

    return jax.shard_map(local_block, mesh=mesh, in_specs=(P(AXES, None), P(AXES), P(None, None), P("ep", None, None), P("ep", None, None)), out_specs=P(AXES, None), check_vma=False)
```
